32 devices in a mesh: patch: 32 (over z, y, x, core).
Axes of the slice: x: 2, y: 2, z: 4, core: 2. Of those that a mesh axis runs over, the one named last changes fastest.
Arguments:
- grid_latent: bfloat16 [131072, 512], P('patch'), may hold values from -6 to 6
- mesh_latent: bfloat16 [10240, 512], P('patch'), may hold values from -6 to 6
- mesh_cotangent: bfloat16 [10240, 512], P('patch'), may hold values from -6 to 6
- grid_rows: int32 [12288], P('patch'), may hold values from 0 to 4095
- mesh_rows: int32 [12288], P('patch'), may hold values from 0 to 319
- counts: int32 [32, 32], P('patch'), may hold values from 1 to 12, as said below
- w1_grid: bfloat16 [512, 512], replicated, may hold values from -0.25 to 0.25
- w1_mesh: bfloat16 [512, 512], replicated, may hold values from -0.25 to 0.25
- bias_one: float32 [512], replicated, may hold values from -3 to 3
- w2: bfloat16 [512, 512], replicated, may hold values from -0.25 to 0.25
Outputs:
- grid_grad: float32 [131072, 512], P('patch')
- mesh_grad: float32 [10240, 512], P('patch')
- w1_grid_grad: float32 [512, 512], replicated
- w1_mesh_grad: float32 [512, 512], replicated
- w2_grad: float32 [512, 512], replicated
- bias_grad: float32 [512], replicated
The draws below stay inside these ranges and needn't reach their ends.
Inputs may be any that keep to these rules, and one draw needn't show every extreme that they name: counts[p, q] of the 12 slots from patch p to owner q are live, the first ones; every row and every column of counts has at least one entry equal to 12. `grid_rows`: padding slots hold arbitrary rows in range.
All inputs are finite; a program needn't handle non-finite values.
Results may differ from the reference program's by a relative error of at most 0.007.
Values may be sent and summed in bfloat16 or wider, within the bound.
A program may use at most 128 MiB of HBM per device.

```python
import jax
import jax.numpy as jnp
from jax import lax

D = 512
MLP_W = 512
C = 12
G_DEV = 4096
M_DEV = 320
SLOTS = 12288
GRID = 131072
MESH = 10240
N_PATCH = 32


def draw_counts(key, part):
    base_key = jax.random.fold_in(key, 7)
    key_base, key_level, key_pairs = jax.random.split(base_key, 3)
    base_load = jax.random.randint(key_base, (N_PATCH, N_PATCH), C // 2, C + 1)
    load_level = jax.random.randint(key_level, (N_PATCH, 1), 2, 5)
    loaded = jnp.maximum(1, base_load * load_level // 4)
    shuffled = jax.random.permutation(key_pairs, N_PATCH)
    full_pair = jnp.arange(N_PATCH)[None, :] == shuffled[:, None]
    return jnp.where(full_pair, C, loaded).astype(jnp.int32)


def place_ends(result, key, least, largest):
    index_at = [jax.random.randint(jax.random.fold_in(key, axis), (), 0, length) for axis, length in enumerate(result.shape)]
    widest = result.shape.index(max(result.shape))
    beside = index_at[:widest] + [(index_at[widest] + 1) % result.shape[widest]] + index_at[widest + 1:]
    return result.at[tuple(index_at)].set(least).at[tuple(beside)].set(largest)


def level_of(stream_key, extent, cuts, smallest, high):
    def one(dim, parts):
        heights = jax.random.uniform(jax.random.fold_in(jax.random.fold_in(stream_key, 6), dim), (parts,), jnp.float32, smallest / len(cuts), high / len(cuts))
        return jnp.repeat(jnp.exp(heights), extent[dim] // parts).reshape((-1,) + (1,) * (len(extent) - dim - 1))

    loudness = one(*cuts[0])
    for cut in cuts[1:]:
        loudness = loudness * one(*cut)
    return loudness


def scatter_about(key, extent, spread, reach, cuts=(), held_as=jnp.bfloat16):
    values = spread * jax.random.normal(key, extent, jnp.float32)
    if cuts:
        values = values * level_of(key, extent, cuts, -0.22, 0.18)
    return jnp.clip(values, -reach, reach).astype(held_as)


def setup_inputs(seed: int = 0) -> dict:
    seeds = jax.random.split(jax.random.key(seed), 11)
    grid_latent = scatter_about(seeds[0], (GRID, D), 1.0, 6.0, ((0, 32),))
    mesh_latent = scatter_about(seeds[1], (MESH, D), 1.0, 6.0, ((0, 32),))
    mesh_cotangent = scatter_about(seeds[2], (MESH, D), 1.0, 6.0, ((0, 32),))
    grid_rows = place_ends(jax.random.randint(seeds[3], (SLOTS,), 0, G_DEV), jax.random.fold_in(seeds[3], 1), 0, G_DEV - 1).astype(jnp.int32)
    mesh_rows = place_ends(jax.random.randint(seeds[4], (SLOTS,), 0, M_DEV), jax.random.fold_in(seeds[4], 1), 0, M_DEV - 1).astype(jnp.int32)
    counts = draw_counts(jax.random.fold_in(seeds[10], 71), 0)
    w1_grid = scatter_about(seeds[6], (D, MLP_W), D ** -0.5, 0.25)
    w1_mesh = scatter_about(seeds[7], (D, MLP_W), D ** -0.5, 0.25)
    bias_one = scatter_about(seeds[8], (MLP_W,), 0.5, 3.0, (), jnp.float32)
    w2 = scatter_about(seeds[9], (MLP_W, D), MLP_W ** -0.5, 0.25)
    return {"grid_latent": grid_latent, "mesh_latent": mesh_latent, "mesh_cotangent": mesh_cotangent, "grid_rows": grid_rows, "mesh_rows": mesh_rows, "counts": counts, "w1_grid": w1_grid, "w1_mesh": w1_mesh, "bias_one": bias_one, "w2": w2}


def reference(grid_latent, mesh_latent, mesh_cotangent, grid_rows, mesh_rows, counts, w1_grid, w1_mesh, bias_one, w2):
    per_patch = N_PATCH * C
    slot_ids = jnp.arange(per_patch, dtype=jnp.int32)
    owners = slot_ids // C
    within = slot_ids % C
    grid_local = grid_rows.reshape(N_PATCH, per_patch)
    mesh_local = mesh_rows.reshape(N_PATCH, per_patch)
    senders = jnp.arange(N_PATCH, dtype=jnp.int32)

    def accumulate(carried, inputs):
        grid_acc, wg_acc, wm_acc, w2_acc, bias_acc = carried
        sender, grid_part, mesh_part, sent_counts = inputs
        grid_index = (owners * G_DEV + grid_part).astype(jnp.int32)
        mesh_index = (sender * M_DEV + mesh_part).astype(jnp.int32)
        live_mask = within < sent_counts[owners]
        grid_in = grid_latent[grid_index]
        mesh_in = mesh_latent[mesh_index]
        grid_proj = jnp.dot(grid_in, w1_grid, preferred_element_type=jnp.float32).astype(jnp.bfloat16)
        before = grid_proj.astype(jnp.float32) + jnp.dot(mesh_in, w1_mesh, preferred_element_type=jnp.float32) + bias_one
        logistic = jax.nn.sigmoid(before)
        hidden = (before * logistic).astype(jnp.bfloat16)
        derivative = logistic * (1.0 + before * (1.0 - logistic))
        out_grad = jnp.where(live_mask[:, None], mesh_cotangent[mesh_index], jnp.zeros((), jnp.bfloat16))
        hid_grad = jnp.dot(out_grad, w2.T, preferred_element_type=jnp.float32)
        pre_grad = (hid_grad * derivative).astype(jnp.bfloat16)
        edge_grid = jnp.dot(pre_grad, w1_grid.T, preferred_element_type=jnp.float32).astype(jnp.bfloat16)
        grid_acc = grid_acc.at[grid_index].add(edge_grid.astype(jnp.float32))
        node_sum = jax.ops.segment_sum(pre_grad.astype(jnp.float32), mesh_part, num_segments=M_DEV)
        mesh_block = jnp.dot(node_sum, w1_mesh.T.astype(jnp.float32), precision=lax.Precision.HIGHEST)
        wg_acc = wg_acc + jnp.dot(grid_in.T, pre_grad, preferred_element_type=jnp.float32)
        wm_acc = wm_acc + jnp.dot(mesh_in.T, pre_grad, preferred_element_type=jnp.float32)
        w2_acc = w2_acc + jnp.dot(hidden.T, out_grad, preferred_element_type=jnp.float32)
        bias_acc = bias_acc + lax.optimization_barrier(jnp.sum(pre_grad.astype(jnp.float32), axis=0))
        return ((grid_acc, wg_acc, wm_acc, w2_acc, bias_acc), mesh_block)
    start = (jnp.zeros((G_DEV * N_PATCH, D), jnp.float32), jnp.zeros((D, MLP_W), jnp.float32), jnp.zeros((D, MLP_W), jnp.float32), jnp.zeros((MLP_W, D), jnp.float32), jnp.zeros((MLP_W,), jnp.float32))
    finals, mesh_blocks = lax.scan(accumulate, start, (senders, grid_local, mesh_local, counts))
    grid_grad, wg_acc, wm_acc, w2_acc, bias_acc = finals
    norm_scale = 1.0 / jnp.sqrt(jnp.float32(N_PATCH * N_PATCH * C))
    mesh_grad = mesh_blocks.reshape(N_PATCH * M_DEV, D)
    return (grid_grad, mesh_grad, wg_acc * norm_scale, wm_acc * norm_scale, w2_acc * norm_scale, bias_acc * norm_scale)
```

```python
import functools
import math

import jax
import jax.numpy as jnp
from jax import lax
from jax.experimental import pallas as pl
from jax.experimental.pallas import tpu as pltpu
from jax.sharding import PartitionSpec as P

BF16 = jnp.bfloat16
F32 = jnp.float32
VMEM_LIMIT = 64 * 1024 * 1024 - 1024 * 1024
MIN_ROWS = 16


def dot(a, b):
    return jnp.dot(a, b, preferred_element_type=F32)


def dot_tn(a, b):
    return lax.dot_general(a, b, (((0,), (0,)), ((), ())), preferred_element_type=F32)


def dot_nt(a, b):
    return lax.dot_general(a, b, (((1,), (1,)), ((), ())), preferred_element_type=F32)


def one_hot(hit):
    return jnp.where(hit, 1.0, 0.0).astype(BF16)


def bit_orders(bits):
    rest = list(range(4, bits))
    if bits < 4:
        return [list(range(bits))] * 3
    return [[0, 1, 2, 3] + rest, [0, 2, 3, 1] + rest, [0, 3, 1, 2] + rest]


def main_kernel(
    n,
    cap,
    cpad,
    grid_any,
    mesh_ref,
    cot_ref,
    grows_ref,
    mcol_ref,
    lcol_ref,
    mrow_ref,
    w1g_ref,
    w1m_ref,
    bias_ref,
    w2_ref,
    edge_out,
    rows_out,
    wsum_out,
    bsum_out,
    mgrad_out,
    glat,
    s_msg,
    r_msg,
    r_rows,
    rows2,
    wide,
    gin,
    pre,
    s_pre,
    r_pre,
    s_bias,
    r_bias,
    acc,
    sbuf,
    rbuf,
    abuf,
    glat_sem,
    phase_send,
    phase_recv,
    red_send,
    red_recv,
    ag_send,
    ag_recv,
):
    me = lax.axis_index("patch")
    width = mesh_ref.shape[1]
    slots = n * cpad
    grid_rows_n = glat.shape[0]
    mesh_n = mesh_ref.shape[0]

    load = pltpu.make_async_copy(grid_any, glat, glat_sem)
    load.start()

    barrier = pltpu.get_barrier_semaphore()

    def greet(k, carry):
        pl.semaphore_signal(barrier, inc=1, device_id=(lax.rem(me + k, n),), device_id_type=pl.DeviceIdType.MESH)
        return carry

    lax.fori_loop(1, n, greet, 0)

    mesh_iota = lax.broadcasted_iota(jnp.int32, (slots, mesh_n), 1)
    mesh_in = dot(one_hot(mcol_ref[...] == mesh_iota), mesh_ref[...]).astype(BF16)
    wide[...] = mesh_in.reshape(n, cpad, width)
    s_msg[:, 0] = wide[:, 0:cap, :]
    cot_in = dot(one_hot(lcol_ref[...] == mesh_iota), cot_ref[...]).astype(BF16)
    wide[...] = cot_in.reshape(n, cpad, width)
    s_msg[:, 1] = wide[:, 0:cap, :]

    pl.semaphore_wait(barrier, n - 1)

    def exchange(phase, src, dst, shared=False):
        def send(k, carry):
            partner = lax.rem(me + k, n)
            pltpu.make_async_remote_copy(
                src_ref=src if shared else src.at[partner],
                dst_ref=dst.at[me],
                send_sem=phase_send.at[phase],
                recv_sem=phase_recv.at[phase],
                device_id=(partner,),
                device_id_type=pl.DeviceIdType.MESH,
            ).start()
            return carry

        lax.fori_loop(1, n, send, 0)

    def arrived(phase, dst):
        part = dst.at[pl.ds(0, n - 1)]
        pltpu.make_async_copy(part, part, phase_recv.at[phase]).wait()

    def left(phase, dst):
        part = dst.at[pl.ds(0, n - 1)]
        pltpu.make_async_copy(part, part, phase_send.at[phase]).wait()

    exchange(0, grows_ref, r_rows)
    exchange(1, s_msg, r_msg)
    r_rows[me] = grows_ref[me]
    r_msg[me] = s_msg[me]
    arrived(0, r_rows)

    def flatten(p, carry):
        rows2[pl.ds(p, 1), :] = r_rows[p].astype(F32)
        return carry

    lax.fori_loop(0, n, flatten, 0)
    table = rows2[...]
    lanes = table.shape[1]
    from_patch = jnp.where(
        lax.broadcasted_iota(jnp.int32, (slots, n), 0) // cpad == lax.broadcasted_iota(jnp.int32, (slots, n), 1), 1.0, 0.0
    )
    spread = jnp.dot(from_patch, table, preferred_element_type=F32, precision=lax.Precision.HIGHEST)
    own_lane = lax.broadcasted_iota(jnp.int32, (slots, lanes), 1) == lax.broadcasted_iota(jnp.int32, (slots, lanes), 0) % cpad
    col = jnp.sum(jnp.where(own_lane, spread, 0.0), axis=1, keepdims=True).astype(jnp.int32)
    to_patch = jnp.where(
        lax.broadcasted_iota(jnp.int32, (n, slots), 1) // cpad == lax.broadcasted_iota(jnp.int32, (n, slots), 0), 1.0, 0.0
    )
    spread_t = lax.dot_general(
        table, to_patch, (((0,), (0,)), ((), ())), preferred_element_type=F32, precision=lax.Precision.HIGHEST
    )
    own_sub = lax.broadcasted_iota(jnp.int32, (lanes, slots), 0) == lax.broadcasted_iota(jnp.int32, (lanes, slots), 1) % cpad
    row = jnp.sum(jnp.where(own_sub, spread_t, 0.0), axis=0, keepdims=True).astype(jnp.int32)
    rows_out[...] = jnp.broadcast_to(row, rows_out.shape)

    load.wait()
    step = min(512, grid_rows_n)
    gin[...] = jnp.zeros_like(gin)

    def gather(i, carry):
        base = pl.multiple_of(i * step, step)
        hit = (col - base) == lax.broadcasted_iota(jnp.int32, (slots, step), 1)
        gin[...] += dot(one_hot(hit), glat[pl.ds(base, step), :])
        return carry

    lax.fori_loop(0, grid_rows_n // step, gather, 0)
    grid_in = gin[...].astype(BF16)
    grid_proj = dot(grid_in, w1g_ref[...]).astype(BF16).astype(F32)

    arrived(1, r_msg)
    wide[...] = jnp.zeros_like(wide)
    wide[:, 0:cap, :] = r_msg[:, 1]
    out_grad = wide[...].reshape(slots, width)
    wide[:, 0:cap, :] = r_msg[:, 0]
    mesh_all = wide[...].reshape(slots, width)
    before = grid_proj + dot(mesh_all, w1m_ref[...]) + bias_ref[...]
    logistic = jax.nn.sigmoid(before)
    hidden = (before * logistic).astype(BF16)
    derivative = logistic * (1.0 + before * (1.0 - logistic))
    pre_f = dot_nt(out_grad, w2_ref[...]) * derivative
    pre_grad = pre_f.astype(BF16)
    pre[...] = pre_grad

    acc[0] = dot_tn(grid_in, pre_grad)
    acc[1] = dot_tn(mesh_all, pre_grad)
    acc[2] = dot_tn(hidden, out_grad)

    bits = n.bit_length() - 1
    orders = bit_orders(bits)
    total = acc.shape[1]
    halvings = 0
    while halvings < bits and (total >> (halvings + 1)) >= MIN_ROWS:
        halvings += 1
    base = [0, 0, 0]

    def partner_of(bit):
        b = lax.rem(me // (1 << bit), 2)
        return b, me + (1 - 2 * b) * (1 << bit)

    def red_copy(s, t, src_at, half, off, partner):
        return pltpu.make_async_remote_copy(
            src_ref=sbuf.at[s, pl.ds(src_at, half), :],
            dst_ref=rbuf.at[s, pl.ds(off, half), :],
            send_sem=red_send.at[s, t],
            recv_sem=red_recv.at[s, t],
            device_id=(partner,),
            device_id_type=pl.DeviceIdType.MESH,
        )

    copies = []

    def start_stage(t):
        started = []
        for s in range(3):
            b, partner = partner_of(orders[s][t])
            if t < halvings:
                half = total >> (t + 1)
                off = total - 2 * half
                give = pl.multiple_of(base[s] + (1 - b) * half, MIN_ROWS)
                keep = pl.multiple_of(base[s] + b * half, MIN_ROWS)
                src_at = give
            else:
                half = total >> halvings
                off = total - half + (t - halvings) * half
                give = keep = base[s]
                src_at = total + (t - halvings) * half
            sbuf[s, pl.ds(src_at, half), :] = acc[s, pl.ds(give, half), :].astype(BF16)
            c = red_copy(s, t, src_at, half, off, partner)
            c.start()
            copies.append(c)
            started.append((c, keep, half, off))
            base[s] = keep
        return started

    def finish_stage(t, started):
        for s in range(3):
            c, keep, half, off = started[s]
            c.wait_recv()
            mine = acc[s, pl.ds(keep, half), :]
            if t >= halvings:
                mine = mine.astype(BF16).astype(F32)
            acc[s, pl.ds(keep, half), :] = mine + rbuf[s, pl.ds(off, half), :].astype(F32)

    started = start_stage(0)

    s_bias[...] = jnp.sum(pre_grad.astype(F32), axis=0, keepdims=True)
    wide[...] = pre_grad.reshape(n, cpad, width)
    s_pre[...] = wide[:, 0:cap, :]
    exchange(2, s_pre, r_pre)
    exchange(3, s_bias, r_bias, shared=True)
    r_pre[me] = s_pre[me]
    r_bias[me] = s_bias[...]
    edge_out[...] = dot_nt(pre[...], w1g_ref[...]).astype(BF16)

    for t in range(bits):
        if t > 0:
            started = start_stage(t)
        finish_stage(t, started)

    ag = []
    for s in range(3):
        size = total >> halvings
        abuf[s, pl.ds(base[s], size), :] = acc[s, pl.ds(base[s], size), :].astype(BF16)
    for t in reversed(range(halvings)):
        row_sends = []
        for s in range(3):
            size = total >> (t + 1)
            b, partner = partner_of(orders[s][t])
            c = pltpu.make_async_remote_copy(
                src_ref=abuf.at[s, pl.ds(base[s], size), :],
                dst_ref=abuf.at[s, pl.ds(base[s], size), :],
                send_sem=ag_send.at[s, t],
                recv_sem=ag_recv.at[s, t],
                device_id=(partner,),
                device_id_type=pl.DeviceIdType.MESH,
            )
            c.start()
            row_sends.append(c)
            ag.append(c)
            base[s] = pl.multiple_of(base[s] - b * size, MIN_ROWS)
        if t == halvings - 1:
            arrived(2, r_pre)
            wide[...] = jnp.zeros_like(wide)
            wide[:, 0:cap, :] = r_pre[...]
            back = wide[...].reshape(slots, width)
            hit = mrow_ref[...] == lax.broadcasted_iota(jnp.int32, (mesh_n, slots), 0)
            node = dot(one_hot(hit), back)
            high = node.astype(BF16)
            low = (node - high.astype(F32)).astype(BF16)
            mgrad_out[...] = dot_nt(high, w1m_ref[...]) + dot_nt(low, w1m_ref[...])
            arrived(3, r_bias)
            bsum_out[...] = jnp.sum(r_bias[...], axis=0)
        for c in row_sends:
            c.wait_recv()
    wsum_out[...] = abuf[...]

    for c in copies + ag:
        c.wait_send()
    left(0, r_rows)
    left(1, r_msg)
    left(2, r_pre)
    left(3, r_bias)


def final_kernel(scale, step, rows_ref, edge_ref, wsum_ref, bsum_ref, mgrad_ref, gg, mg, wg, wm, w2g, bg):
    i = pl.program_id(0)
    slots = rows_ref.shape[1]
    hit = (rows_ref[0:1, :] - i * step) == lax.broadcasted_iota(jnp.int32, (step, slots), 0)
    gg[...] = dot(one_hot(hit), edge_ref[...])
    wg[...] = wsum_ref[0].astype(F32) * scale
    wm[...] = wsum_ref[1].astype(F32) * scale
    w2g[...] = wsum_ref[2].astype(F32) * scale

    @pl.when(i == 0)
    def _():
        mg[...] = mgrad_ref[...]
        bg[...] = bsum_ref[...] * scale


def body(n, grid_latent, mesh_latent, mesh_cotangent, grid_rows, mesh_rows, counts, w1_grid, w1_mesh, bias_one, w2):
    slot_count = grid_rows.shape[0]
    cap = slot_count // n
    cpad = -(-cap // 16) * 16
    lanes = -(-cpad // 128) * 128
    width = mesh_latent.shape[1]
    hid = w1_grid.shape[1]
    grid_n = grid_latent.shape[0]
    mesh_n = mesh_latent.shape[0]
    slots = n * cpad
    bits = n.bit_length() - 1

    pad = ((0, 0), (0, cpad - cap))
    mrows = jnp.pad(mesh_rows.reshape(n, cap), pad, constant_values=-1)
    live = jnp.arange(cpad, dtype=jnp.int32)[None, :] < counts[0][:, None]
    lrows = jnp.where(live, mrows, -1)
    grows = jnp.pad(grid_rows.reshape(n, 1, cap), ((0, 0), (0, 0), (0, lanes - cap)), constant_values=-1)

    vm = pl.BlockSpec(memory_space=pltpu.VMEM)
    extra = (max(0, bits - int(math.log2(width // MIN_ROWS))) + 1) * MIN_ROWS
    edge, rows, wsum, bsum, mgrad = pl.pallas_call(
        functools.partial(main_kernel, n, cap, cpad),
        out_shape=(
            jax.ShapeDtypeStruct((slots, width), BF16),
            jax.ShapeDtypeStruct((8, slots), jnp.int32),
            jax.ShapeDtypeStruct((3, width, hid), BF16),
            jax.ShapeDtypeStruct((1, hid), F32),
            jax.ShapeDtypeStruct((mesh_n, width), F32),
        ),
        in_specs=[pl.BlockSpec(memory_space=pl.ANY)] + [vm] * 10,
        out_specs=(vm,) * 5,
        scratch_shapes=[
            pltpu.VMEM((grid_n, width), BF16),
            pltpu.VMEM((n, 2, cap, width), BF16),
            pltpu.VMEM((n, 2, cap, width), BF16),
            pltpu.VMEM((n, 1, lanes), jnp.int32),
            pltpu.VMEM((n, lanes), F32),
            pltpu.VMEM((n, cpad, width), BF16),
            pltpu.VMEM((slots, width), F32),
            pltpu.VMEM((slots, hid), BF16),
            pltpu.VMEM((n, cap, hid), BF16),
            pltpu.VMEM((n, cap, hid), BF16),
            pltpu.VMEM((1, hid), F32),
            pltpu.VMEM((n, 1, hid), F32),
            pltpu.VMEM((3, width, hid), F32),
            pltpu.VMEM((3, width + extra, hid), BF16),
            pltpu.VMEM((3, width + extra, hid), BF16),
            pltpu.VMEM((3, width, hid), BF16),
            pltpu.SemaphoreType.DMA,
            pltpu.SemaphoreType.DMA((4,)),
            pltpu.SemaphoreType.DMA((4,)),
            pltpu.SemaphoreType.DMA((3, bits)),
            pltpu.SemaphoreType.DMA((3, bits)),
            pltpu.SemaphoreType.DMA((3, bits)),
            pltpu.SemaphoreType.DMA((3, bits)),
        ],
        compiler_params=pltpu.CompilerParams(
            collective_id=0, has_side_effects=True, vmem_limit_bytes=VMEM_LIMIT
        ),
    )(
        grid_latent,
        mesh_latent,
        mesh_cotangent,
        grows,
        mrows.reshape(slots, 1),
        lrows.reshape(slots, 1),
        mrows.reshape(1, slots),
        w1_grid,
        w1_mesh,
        bias_one.reshape(1, hid),
        w2,
    )

    step = min(512, grid_n)
    steps = grid_n // step
    part = width // steps
    scale = 1.0 / math.sqrt(n * slot_count)
    whole = lambda *shape: pl.BlockSpec(shape, lambda i: (0,) * len(shape))
    gg, mg, wg, wm, w2g, bg = pl.pallas_call(
        functools.partial(final_kernel, scale, step),
        grid=(steps,),
        out_shape=(
            jax.ShapeDtypeStruct((grid_n, width), F32),
            jax.ShapeDtypeStruct((mesh_n, width), F32),
            jax.ShapeDtypeStruct((width, hid), F32),
            jax.ShapeDtypeStruct((width, hid), F32),
            jax.ShapeDtypeStruct((width, hid), F32),
            jax.ShapeDtypeStruct((1, hid), F32),
        ),
        in_specs=[
            whole(8, slots),
            whole(slots, width),
            pl.BlockSpec((3, part, hid), lambda i: (0, i, 0)),
            whole(1, hid),
            whole(mesh_n, width),
        ],
        out_specs=(
            pl.BlockSpec((step, width), lambda i: (i, 0)),
            whole(mesh_n, width),
            pl.BlockSpec((part, hid), lambda i: (i, 0)),
            pl.BlockSpec((part, hid), lambda i: (i, 0)),
            pl.BlockSpec((part, hid), lambda i: (i, 0)),
            whole(1, hid),
        ),
        compiler_params=pltpu.CompilerParams(vmem_limit_bytes=VMEM_LIMIT),
    )(rows, edge, wsum, bsum, mgrad)
    return gg, mg, wg, wm, w2g, bg.reshape(hid)


def solution(mesh):
    return jax.shard_map(
        functools.partial(body, mesh.shape["patch"]),
        mesh=mesh,
        in_specs=(
            P("patch", None),
            P("patch", None),
            P("patch", None),
            P("patch"),
            P("patch"),
            P("patch", None),
            P(),
            P(),
            P(),
            P(),
        ),
        out_specs=(P("patch", None), P("patch", None), P(), P(), P(), P()),
        check_vma=False,
    )
```

```python
import functools
import math

import jax
import jax.numpy as jnp
from jax import lax
from jax.experimental import pallas as pl
from jax.experimental.pallas import tpu as pltpu
from jax.sharding import PartitionSpec as P

BF16 = jnp.bfloat16
F32 = jnp.float32
VMEM_LIMIT = 64 * 1024 * 1024 - 1024 * 1024
MIN_ROWS = 16


def dot(a, b):
    return jnp.dot(a, b, preferred_element_type=F32)


def dot_tn(a, b):
    return lax.dot_general(a, b, (((0,), (0,)), ((), ())), preferred_element_type=F32)


def dot_nt(a, b):
    return lax.dot_general(a, b, (((1,), (1,)), ((), ())), preferred_element_type=F32)


def one_hot(hit):
    return jnp.where(hit, 1.0, 0.0).astype(BF16)


def bit_orders(bits):
    rest = list(range(4, bits))
    if bits < 4:
        return [list(range(bits))] * 3
    return [[0, 1, 2, 3] + rest, [0, 2, 3, 1] + rest, [0, 3, 1, 2] + rest]


def main_kernel(
    n,
    cap,
    cpad,
    grid_any,
    mesh_ref,
    cot_ref,
    grows_ref,
    mrows_ref,
    counts_ref,
    w1g_any,
    w1m_any,
    bias_ref,
    w2_any,
    edge_out,
    rows_out,
    wsum_out,
    bsum_out,
    mgrad_out,
    glat,
    w1g_ref,
    w1m_ref,
    w2_ref,
    s_rows,
    mhot,
    s_msg,
    r_msg,
    r_rows,
    rows2,
    wide,
    gin,
    pre,
    s_pre,
    r_pre,
    s_bias,
    r_bias,
    acc,
    sbuf,
    rbuf,
    abuf,
    glat_sem,
    weight_sem,
    phase_send,
    phase_recv,
    red_send,
    red_recv,
    ag_send,
    ag_recv,
):
    me = lax.axis_index("patch")
    width = mesh_ref.shape[1]
    slots = n * cpad
    grid_rows_n = glat.shape[0]
    mesh_n = mesh_ref.shape[0]

    load = pltpu.make_async_copy(grid_any, glat, glat_sem)
    loads = [
        pltpu.make_async_copy(src, dst, weight_sem.at[i])
        for i, (src, dst) in enumerate(((w1g_any, w1g_ref), (w1m_any, w1m_ref), (w2_any, w2_ref)))
    ]

    barrier = pltpu.get_barrier_semaphore()

    def greet(k, carry):
        pl.semaphore_signal(barrier, inc=1, device_id=(lax.rem(me + k, n),), device_id_type=pl.DeviceIdType.MESH)
        return carry

    lax.fori_loop(1, n, greet, 0)

    for c in loads:
        c.start()
    load.start()

    lanes = rows2.shape[1]
    count = grows_ref.shape[1]
    chunks = width // 128
    slot_id = lax.broadcasted_iota(jnp.int32, (slots, 1), 0)
    slot_patch = slot_id // cpad
    slot_in = slot_id % cpad
    at = lax.broadcasted_iota(jnp.int32, (n, count), 1) - cap * lax.broadcasted_iota(jnp.int32, (n, count), 0)
    own_part = (at >= 0) & (at < cap)
    lane_of = lax.broadcasted_iota(jnp.int32, (count, lanes), 0) % cap == lax.broadcasted_iota(jnp.int32, (count, lanes), 1)
    lane_of = jnp.where(lane_of, 1.0, 0.0)
    in_cap = lax.broadcasted_iota(jnp.int32, (n, lanes), 1) < cap
    from_patch = jnp.where(slot_patch == lax.broadcasted_iota(jnp.int32, (slots, n), 1), 1.0, 0.0)
    own_lane = lax.broadcasted_iota(jnp.int32, (slots, lanes), 1) == slot_in

    def table_of(ref):
        spread = jnp.where(own_part, ref[...].astype(F32), 0.0)
        out = jnp.dot(spread, lane_of, preferred_element_type=F32, precision=lax.Precision.HIGHEST)
        return jnp.where(in_cap, out, -1.0)

    def column_of(table):
        spread = jnp.dot(from_patch, table, preferred_element_type=F32, precision=lax.Precision.HIGHEST)
        return jnp.sum(jnp.where(own_lane, spread, 0.0), axis=1, keepdims=True).astype(jnp.int32)

    rows2[...] = table_of(grows_ref)

    def split(p, carry):
        s_rows[p] = rows2[pl.ds(p, 1), :].astype(jnp.int32)
        return carry

    lax.fori_loop(0, n, split, 0)
    mcol = column_of(table_of(mrows_ref))
    counted = jnp.where(
        slot_patch == lax.broadcasted_iota(jnp.int32, (slots, n), 1), counts_ref[...].astype(F32), 0.0
    )
    live = slot_in.astype(F32) < jnp.sum(counted, axis=1, keepdims=True)
    lcol = jnp.where(live, mcol, -1)
    mesh_iota = lax.broadcasted_iota(jnp.int32, (slots, mesh_n), 1)
    mhot[...] = one_hot(mcol == mesh_iota)

    def pack(ref, first):
        for j in range(chunks):
            ref[:, (first + j) * cap : (first + j + 1) * cap, :] = wide[:, 0:cap, j * 128 : (j + 1) * 128]

    def unpack(ref, first):
        for j in range(chunks):
            wide[:, 0:cap, j * 128 : (j + 1) * 128] = ref[:, (first + j) * cap : (first + j + 1) * cap, :]

    wide[...] = dot(mhot[...], mesh_ref[...]).astype(BF16).reshape(n, cpad, width)
    pack(s_msg, 0)
    wide[...] = dot(one_hot(lcol == mesh_iota), cot_ref[...]).astype(BF16).reshape(n, cpad, width)
    pack(s_msg, chunks)

    pl.semaphore_wait(barrier, n - 1)

    def exchange(phase, src, dst, shared=False, first=1, last=n):
        def send(k, carry):
            partner = lax.rem(me + k, n)
            pltpu.make_async_remote_copy(
                src_ref=src if shared else src.at[partner],
                dst_ref=dst.at[me],
                send_sem=phase_send.at[phase],
                recv_sem=phase_recv.at[phase],
                device_id=(partner,),
                device_id_type=pl.DeviceIdType.MESH,
            ).start()
            return carry

        lax.fori_loop(first, last, send, 0)

    def arrived(phase, dst):
        part = dst.at[pl.ds(0, n - 1)]
        pltpu.make_async_copy(part, part, phase_recv.at[phase]).wait()

    def left(phase, dst):
        part = dst.at[pl.ds(0, n - 1)]
        pltpu.make_async_copy(part, part, phase_send.at[phase]).wait()

    exchange(0, s_rows, r_rows)
    exchange(1, s_msg, r_msg)
    r_rows[me] = s_rows[me]
    r_msg[me] = s_msg[me]
    arrived(0, r_rows)

    def flatten(p, carry):
        rows2[pl.ds(p, 1), :] = r_rows[p].astype(F32)
        return carry

    lax.fori_loop(0, n, flatten, 0)
    table = rows2[...]
    col = column_of(table)
    to_patch = jnp.where(
        lax.broadcasted_iota(jnp.int32, (n, slots), 1) // cpad == lax.broadcasted_iota(jnp.int32, (n, slots), 0), 1.0, 0.0
    )
    spread_t = lax.dot_general(
        table, to_patch, (((0,), (0,)), ((), ())), preferred_element_type=F32, precision=lax.Precision.HIGHEST
    )
    own_sub = lax.broadcasted_iota(jnp.int32, (lanes, slots), 0) == lax.broadcasted_iota(jnp.int32, (lanes, slots), 1) % cpad
    row = jnp.sum(jnp.where(own_sub, spread_t, 0.0), axis=0, keepdims=True).astype(jnp.int32)
    rows_out[...] = jnp.broadcast_to(row, rows_out.shape)

    load.wait()
    for c in loads:
        c.wait()
    step = min(512, grid_rows_n)
    gin[...] = jnp.zeros_like(gin)

    def gather(i, carry):
        base = pl.multiple_of(i * step, step)
        hit = (col - base) == lax.broadcasted_iota(jnp.int32, (slots, step), 1)
        gin[...] += dot(one_hot(hit), glat[pl.ds(base, step), :])
        return carry

    lax.fori_loop(0, grid_rows_n // step, gather, 0)
    grid_in = gin[...].astype(BF16)
    grid_proj = dot(grid_in, w1g_ref[...]).astype(BF16).astype(F32)

    arrived(1, r_msg)
    wide[...] = jnp.zeros_like(wide)
    unpack(r_msg, chunks)
    out_grad = wide[...].reshape(slots, width)
    unpack(r_msg, 0)
    mesh_all = wide[...].reshape(slots, width)
    before = grid_proj + dot(mesh_all, w1m_ref[...]) + bias_ref[...]
    logistic = jax.nn.sigmoid(before)
    hidden = (before * logistic).astype(BF16)
    derivative = logistic * (1.0 + before * (1.0 - logistic))
    pre_f = dot_nt(out_grad, w2_ref[...]) * derivative
    pre_grad = pre_f.astype(BF16)
    pre[...] = pre_grad

    terms = ((grid_in, pre_grad), (mesh_all, pre_grad), (hidden, out_grad))

    bits = n.bit_length() - 1
    orders = bit_orders(bits)
    total = acc.shape[1]
    halvings = 0
    while halvings < bits and (total >> (halvings + 1)) >= MIN_ROWS:
        halvings += 1
    base = [0, 0, 0]

    def partner_of(bit):
        b = lax.rem(me // (1 << bit), 2)
        return b, me + (1 - 2 * b) * (1 << bit)

    def red_copy(s, t, src_at, half, off, partner):
        return pltpu.make_async_remote_copy(
            src_ref=sbuf.at[s, pl.ds(src_at, half), :],
            dst_ref=rbuf.at[s, pl.ds(off, half), :],
            send_sem=red_send.at[s, t],
            recv_sem=red_recv.at[s, t],
            device_id=(partner,),
            device_id_type=pl.DeviceIdType.MESH,
        )

    copies = []

    def start_stage(t):
        started = []
        for s in range(3):
            if t == 0:
                acc[s] = dot_tn(*terms[s])
            b, partner = partner_of(orders[s][t])
            if t < halvings:
                half = total >> (t + 1)
                off = total - 2 * half
                give = pl.multiple_of(base[s] + (1 - b) * half, MIN_ROWS)
                keep = pl.multiple_of(base[s] + b * half, MIN_ROWS)
                src_at = give
            else:
                half = total >> halvings
                off = total - half + (t - halvings) * half
                give = keep = base[s]
                src_at = total + (t - halvings) * half
            sbuf[s, pl.ds(src_at, half), :] = acc[s, pl.ds(give, half), :].astype(BF16)
            c = red_copy(s, t, src_at, half, off, partner)
            c.start()
            copies.append(c)
            started.append((c, keep, half, off))
            base[s] = keep
        return started

    def finish_stage(t, started):
        for s in range(3):
            c, keep, half, off = started[s]
            c.wait_recv()
            mine = acc[s, pl.ds(keep, half), :]
            if t >= halvings:
                mine = mine.astype(BF16).astype(F32)
            acc[s, pl.ds(keep, half), :] = mine + rbuf[s, pl.ds(off, half), :].astype(F32)

    started = start_stage(0)

    s_bias[...] = jnp.sum(pre_grad.astype(F32), axis=0, keepdims=True)
    wide[...] = pre_grad.reshape(n, cpad, width)
    pack(s_pre, 0)
    exchange(3, s_bias, r_bias, shared=True)
    r_pre[me] = s_pre[me]
    r_bias[me] = s_bias[...]
    edge_out[...] = dot_nt(pre[...], w1g_ref[...]).astype(BF16)

    pieces = bits + 2
    cuts = [1 + (n - 1) * i // pieces for i in range(pieces + 1)]
    for t in range(bits):
        if t > 0:
            started = start_stage(t)
        exchange(2, s_pre, r_pre, first=cuts[t], last=cuts[t + 1])
        finish_stage(t, started)

    ag = []
    for s in range(3):
        size = total >> halvings
        abuf[s, pl.ds(base[s], size), :] = acc[s, pl.ds(base[s], size), :].astype(BF16)
    for t in reversed(range(halvings)):
        row_sends = []
        for s in range(3):
            size = total >> (t + 1)
            b, partner = partner_of(orders[s][t])
            c = pltpu.make_async_remote_copy(
                src_ref=abuf.at[s, pl.ds(base[s], size), :],
                dst_ref=abuf.at[s, pl.ds(base[s], size), :],
                send_sem=ag_send.at[s, t],
                recv_sem=ag_recv.at[s, t],
                device_id=(partner,),
                device_id_type=pl.DeviceIdType.MESH,
            )
            c.start()
            row_sends.append(c)
            ag.append(c)
            base[s] = pl.multiple_of(base[s] - b * size, MIN_ROWS)
        if t >= halvings - 2:
            i = bits + halvings - 1 - t
            exchange(2, s_pre, r_pre, first=cuts[i], last=cuts[i + 1])
        if t == 0:
            arrived(2, r_pre)
            wide[...] = jnp.zeros_like(wide)
            unpack(r_pre, 0)
            back = wide[...].reshape(slots, width)
            node = dot_tn(mhot[...], back)
            high = node.astype(BF16)
            low = (node - high.astype(F32)).astype(BF16)
            mgrad_out[...] = dot_nt(high, w1m_ref[...]) + dot_nt(low, w1m_ref[...])
            arrived(3, r_bias)
            bsum_out[...] = jnp.sum(r_bias[...], axis=0)
        for c in row_sends:
            c.wait_recv()
    wsum_out[...] = abuf[...]

    for c in copies + ag:
        c.wait_send()
    left(0, r_rows)
    left(1, r_msg)
    left(2, r_pre)
    left(3, r_bias)


def final_kernel(scale, step, rows_ref, edge_ref, wsum_ref, bsum_ref, mgrad_ref, gg, mg, wg, wm, w2g, bg):
    i = pl.program_id(0)
    slots = rows_ref.shape[1]
    hit = (rows_ref[0:1, :] - i * step) == lax.broadcasted_iota(jnp.int32, (step, slots), 0)
    gg[...] = dot(one_hot(hit), edge_ref[...])
    wg[...] = wsum_ref[0].astype(F32) * scale
    wm[...] = wsum_ref[1].astype(F32) * scale
    w2g[...] = wsum_ref[2].astype(F32) * scale

    @pl.when(i == 0)
    def _():
        mg[...] = mgrad_ref[...]
        bg[...] = bsum_ref[...] * scale


def body(n, grid_latent, mesh_latent, mesh_cotangent, grid_rows, mesh_rows, counts, w1_grid, w1_mesh, bias_one, w2):
    slot_count = grid_rows.shape[0]
    cap = slot_count // n
    cpad = -(-cap // 16) * 16
    lanes = -(-cpad // 128) * 128
    width = mesh_latent.shape[1]
    hid = w1_grid.shape[1]
    grid_n = grid_latent.shape[0]
    mesh_n = mesh_latent.shape[0]
    slots = n * cpad
    bits = n.bit_length() - 1

    vm = pl.BlockSpec(memory_space=pltpu.VMEM)
    hbm = pl.BlockSpec(memory_space=pl.ANY)
    chunks = width // 128
    extra = (max(0, bits - int(math.log2(width // MIN_ROWS))) + 1) * MIN_ROWS
    edge, rows, wsum, bsum, mgrad = pl.pallas_call(
        functools.partial(main_kernel, n, cap, cpad),
        out_shape=(
            jax.ShapeDtypeStruct((slots, width), BF16),
            jax.ShapeDtypeStruct((8, slots), jnp.int32),
            jax.ShapeDtypeStruct((3, width, hid), BF16),
            jax.ShapeDtypeStruct((1, hid), F32),
            jax.ShapeDtypeStruct((mesh_n, width), F32),
        ),
        in_specs=[hbm, vm, vm, vm, vm, vm, hbm, hbm, vm, hbm],
        out_specs=(vm,) * 5,
        scratch_shapes=[
            pltpu.VMEM((grid_n, width), BF16),
            pltpu.VMEM((width, hid), BF16),
            pltpu.VMEM((width, hid), BF16),
            pltpu.VMEM((hid, width), BF16),
            pltpu.VMEM((n, 1, lanes), jnp.int32),
            pltpu.VMEM((slots, mesh_n), BF16),
            pltpu.VMEM((n, 2 * chunks * cap, 128), BF16),
            pltpu.VMEM((n, 2 * chunks * cap, 128), BF16),
            pltpu.VMEM((n, 1, lanes), jnp.int32),
            pltpu.VMEM((n, lanes), F32),
            pltpu.VMEM((n, cpad, width), BF16),
            pltpu.VMEM((slots, width), F32),
            pltpu.VMEM((slots, hid), BF16),
            pltpu.VMEM((n, chunks * cap, 128), BF16),
            pltpu.VMEM((n, chunks * cap, 128), BF16),
            pltpu.VMEM((1, hid), F32),
            pltpu.VMEM((n, 1, hid), F32),
            pltpu.VMEM((3, width, hid), F32),
            pltpu.VMEM((3, width + extra, hid), BF16),
            pltpu.VMEM((3, width + extra, hid), BF16),
            pltpu.VMEM((3, width, hid), BF16),
            pltpu.SemaphoreType.DMA,
            pltpu.SemaphoreType.DMA((3,)),
            pltpu.SemaphoreType.DMA((4,)),
            pltpu.SemaphoreType.DMA((4,)),
            pltpu.SemaphoreType.DMA((3, bits)),
            pltpu.SemaphoreType.DMA((3, bits)),
            pltpu.SemaphoreType.DMA((3, bits)),
            pltpu.SemaphoreType.DMA((3, bits)),
        ],
        compiler_params=pltpu.CompilerParams(
            collective_id=0, has_side_effects=True, vmem_limit_bytes=VMEM_LIMIT
        ),
    )(
        grid_latent,
        mesh_latent,
        mesh_cotangent,
        grid_rows.reshape(1, slot_count),
        mesh_rows.reshape(1, slot_count),
        counts,
        w1_grid,
        w1_mesh,
        bias_one.reshape(1, hid),
        w2,
    )

    step = min(512, grid_n)
    steps = grid_n // step
    part = width // steps
    scale = 1.0 / math.sqrt(n * slot_count)
    whole = lambda *shape: pl.BlockSpec(shape, lambda i: (0,) * len(shape))
    gg, mg, wg, wm, w2g, bg = pl.pallas_call(
        functools.partial(final_kernel, scale, step),
        grid=(steps,),
        out_shape=(
            jax.ShapeDtypeStruct((grid_n, width), F32),
            jax.ShapeDtypeStruct((mesh_n, width), F32),
            jax.ShapeDtypeStruct((width, hid), F32),
            jax.ShapeDtypeStruct((width, hid), F32),
            jax.ShapeDtypeStruct((width, hid), F32),
            jax.ShapeDtypeStruct((1, hid), F32),
        ),
        in_specs=[
            whole(8, slots),
            whole(slots, width),
            pl.BlockSpec((3, part, hid), lambda i: (0, i, 0)),
            whole(1, hid),
            whole(mesh_n, width),
        ],
        out_specs=(
            pl.BlockSpec((step, width), lambda i: (i, 0)),
            whole(mesh_n, width),
            pl.BlockSpec((part, hid), lambda i: (i, 0)),
            pl.BlockSpec((part, hid), lambda i: (i, 0)),
            pl.BlockSpec((part, hid), lambda i: (i, 0)),
            whole(1, hid),
        ),
        compiler_params=pltpu.CompilerParams(vmem_limit_bytes=VMEM_LIMIT),
    )(rows, edge, wsum, bsum, mgrad)
    return gg, mg, wg, wm, w2g, bg.reshape(hid)


def solution(mesh):
    return jax.shard_map(
        functools.partial(body, mesh.shape["patch"]),
        mesh=mesh,
        in_specs=(
            P("patch", None),
            P("patch", None),
            P("patch", None),
            P("patch"),
            P("patch"),
            P("patch", None),
            P(),
            P(),
            P(),
            P(),
        ),
        out_specs=(P("patch", None), P("patch", None), P(), P(), P(), P()),
        check_vma=False,
    )
```

```python
import functools
import math

import jax
import jax.numpy as jnp
from jax import lax
from jax.experimental import pallas as pl
from jax.experimental.pallas import tpu as pltpu
from jax.sharding import PartitionSpec as P

BF16 = jnp.bfloat16
F32 = jnp.float32
VMEM_LIMIT = 64 * 1024 * 1024 - 1024 * 1024
MIN_ROWS = 16


def dot(a, b):
    return jnp.dot(a, b, preferred_element_type=F32)


def dot_tn(a, b):
    return lax.dot_general(a, b, (((0,), (0,)), ((), ())), preferred_element_type=F32)


def dot_nt(a, b):
    return lax.dot_general(a, b, (((1,), (1,)), ((), ())), preferred_element_type=F32)


def one_hot(hit):
    return jnp.where(hit, 1.0, 0.0).astype(BF16)


def bit_orders(bits):
    if bits < 4:
        return [list(range(bits))] * 6
    rest = list(range(4, bits))
    return [[0, *order, *rest] for order in ((1, 2, 3), (2, 3, 1), (3, 1, 2), (1, 3, 2), (2, 1, 3), (3, 2, 1))]


def main_kernel(
    n,
    cap,
    cpad,
    grid_any,
    mesh_ref,
    cot_ref,
    grows_ref,
    mrows_ref,
    counts_ref,
    w1g_any,
    w1m_any,
    bias_ref,
    w2_any,
    edge_out,
    rows_out,
    wsum_out,
    bsum_out,
    mgrad_out,
    glat,
    w1g_ref,
    w1m_ref,
    w2_ref,
    s_rows,
    mhot,
    s_msg,
    r_msg,
    r_rows,
    rows2,
    wide,
    gin,
    pre,
    s_pre,
    r_pre,
    s_bias,
    r_bias,
    acc,
    sbuf,
    rbuf,
    abuf,
    glat_sem,
    weight_sem,
    phase_send,
    phase_recv,
    red_send,
    red_recv,
    ag_send,
    ag_recv,
):
    me = lax.axis_index("patch")
    width = mesh_ref.shape[1]
    slots = n * cpad
    grid_rows_n = glat.shape[0]
    mesh_n = mesh_ref.shape[0]

    load = pltpu.make_async_copy(grid_any, glat, glat_sem)
    loads = [
        pltpu.make_async_copy(src, dst, weight_sem.at[i])
        for i, (src, dst) in enumerate(((w1g_any, w1g_ref), (w1m_any, w1m_ref), (w2_any, w2_ref)))
    ]

    barrier = pltpu.get_barrier_semaphore()

    def greet(k, carry):
        pl.semaphore_signal(barrier, inc=1, device_id=(lax.rem(me + k, n),), device_id_type=pl.DeviceIdType.MESH)
        return carry

    lax.fori_loop(1, n, greet, 0)

    for c in loads:
        c.start()
    load.start()

    lanes = rows2.shape[1]
    count = grows_ref.shape[0]
    chunks = width // 128
    slot_id = lax.broadcasted_iota(jnp.int32, (slots, 1), 0)
    slot_patch = slot_id // cpad
    slot_in = slot_id % cpad
    at = lax.broadcasted_iota(jnp.int32, (n, count), 1) - cap * lax.broadcasted_iota(jnp.int32, (n, count), 0)
    own_part = (at >= 0) & (at < cap)
    lane_of = lax.broadcasted_iota(jnp.int32, (count, lanes), 0) % cap == lax.broadcasted_iota(jnp.int32, (count, lanes), 1)
    lane_of = jnp.where(lane_of, 1.0, 0.0)
    in_cap = lax.broadcasted_iota(jnp.int32, (n, lanes), 1) < cap
    from_patch = jnp.where(slot_patch == lax.broadcasted_iota(jnp.int32, (slots, n), 1), 1.0, 0.0)
    own_lane = lax.broadcasted_iota(jnp.int32, (slots, lanes), 1) == slot_in

    def table_of(ref):
        spread = jnp.where(own_part, ref[...].reshape(1, count).astype(F32), 0.0)
        out = jnp.dot(spread, lane_of, preferred_element_type=F32, precision=lax.Precision.HIGHEST)
        return jnp.where(in_cap, out, -1.0)

    def column_of(table):
        spread = jnp.dot(from_patch, table, preferred_element_type=F32, precision=lax.Precision.HIGHEST)
        return jnp.sum(jnp.where(own_lane, spread, 0.0), axis=1, keepdims=True).astype(jnp.int32)

    rows2[...] = table_of(grows_ref)

    def split(p, carry):
        s_rows[p] = rows2[pl.ds(p, 1), :].astype(jnp.int32)
        return carry

    lax.fori_loop(0, n, split, 0)
    mcol = column_of(table_of(mrows_ref))
    counted = jnp.where(
        slot_patch == lax.broadcasted_iota(jnp.int32, (slots, n), 1), counts_ref[...].astype(F32), 0.0
    )
    live = slot_in.astype(F32) < jnp.sum(counted, axis=1, keepdims=True)
    lcol = jnp.where(live, mcol, -1)
    mesh_iota = lax.broadcasted_iota(jnp.int32, (slots, mesh_n), 1)
    mhot[...] = one_hot(mcol == mesh_iota)

    def pack(ref, first):
        for j in range(chunks):
            ref[:, (first + j) * cap : (first + j + 1) * cap, :] = wide[:, 0:cap, j * 128 : (j + 1) * 128]

    def unpack(ref, first):
        for j in range(chunks):
            wide[:, 0:cap, j * 128 : (j + 1) * 128] = ref[:, (first + j) * cap : (first + j + 1) * cap, :]

    wide[...] = dot(mhot[...], mesh_ref[...]).astype(BF16).reshape(n, cpad, width)
    pack(s_msg, 0)
    wide[...] = dot(one_hot(lcol == mesh_iota), cot_ref[...]).astype(BF16).reshape(n, cpad, width)
    pack(s_msg, chunks)

    pl.semaphore_wait(barrier, n - 1)

    def exchange(phase, src, dst, shared=False, first=1, last=n):
        def send(k, carry):
            partner = lax.rem(me + k, n)
            pltpu.make_async_remote_copy(
                src_ref=src if shared else src.at[partner],
                dst_ref=dst.at[me],
                send_sem=phase_send.at[phase],
                recv_sem=phase_recv.at[phase],
                device_id=(partner,),
                device_id_type=pl.DeviceIdType.MESH,
            ).start()
            return carry

        lax.fori_loop(first, last, send, 0)

    def arrived(phase, dst):
        part = dst.at[pl.ds(0, n - 1)]
        pltpu.make_async_copy(part, part, phase_recv.at[phase]).wait()

    def left(phase, dst):
        part = dst.at[pl.ds(0, n - 1)]
        pltpu.make_async_copy(part, part, phase_send.at[phase]).wait()

    exchange(0, s_rows, r_rows)
    exchange(1, s_msg, r_msg)
    r_rows[me] = s_rows[me]
    r_msg[me] = s_msg[me]
    arrived(0, r_rows)

    def flatten(p, carry):
        rows2[pl.ds(p, 1), :] = r_rows[p].astype(F32)
        return carry

    lax.fori_loop(0, n, flatten, 0)
    table = rows2[...]
    col = column_of(table)
    to_patch = jnp.where(
        lax.broadcasted_iota(jnp.int32, (n, slots), 1) // cpad == lax.broadcasted_iota(jnp.int32, (n, slots), 0), 1.0, 0.0
    )
    spread_t = lax.dot_general(
        table, to_patch, (((0,), (0,)), ((), ())), preferred_element_type=F32, precision=lax.Precision.HIGHEST
    )
    own_sub = lax.broadcasted_iota(jnp.int32, (lanes, slots), 0) == lax.broadcasted_iota(jnp.int32, (lanes, slots), 1) % cpad
    row = jnp.sum(jnp.where(own_sub, spread_t, 0.0), axis=0, keepdims=True).astype(jnp.int32)
    rows_out[...] = jnp.broadcast_to(row, rows_out.shape)

    load.wait()
    for c in loads:
        c.wait()
    step = min(512, grid_rows_n)
    gin[...] = jnp.zeros_like(gin)

    def gather(i, carry):
        base = pl.multiple_of(i * step, step)
        hit = (col - base) == lax.broadcasted_iota(jnp.int32, (slots, step), 1)
        gin[...] += dot(one_hot(hit), glat[pl.ds(base, step), :])
        return carry

    lax.fori_loop(0, grid_rows_n // step, gather, 0)
    grid_in = gin[...].astype(BF16)
    grid_proj = dot(grid_in, w1g_ref[...]).astype(BF16).astype(F32)

    arrived(1, r_msg)
    wide[...] = jnp.zeros_like(wide)
    unpack(r_msg, chunks)
    out_grad = wide[...].reshape(slots, width)
    unpack(r_msg, 0)
    mesh_all = wide[...].reshape(slots, width)
    before = grid_proj + dot(mesh_all, w1m_ref[...]) + bias_ref[...]
    logistic = jax.nn.sigmoid(before)
    hidden = (before * logistic).astype(BF16)
    derivative = logistic * (1.0 + before * (1.0 - logistic))
    pre_f = dot_nt(out_grad, w2_ref[...]) * derivative
    pre_grad = pre_f.astype(BF16)
    pre[...] = pre_grad

    terms = ((grid_in, pre_grad), (mesh_all, pre_grad), (hidden, out_grad))

    bits = n.bit_length() - 1
    orders = bit_orders(bits)
    total = acc.shape[1]
    halvings = 0
    while halvings < bits and (total >> (halvings + 1)) >= MIN_ROWS:
        halvings += 1
    base = [0] * 6

    def partner_of(bit):
        b = lax.rem(me // (1 << bit), 2)
        return b, me + (1 - 2 * b) * (1 << bit)

    def red_copy(s, t, src_at, half, off, partner):
        return pltpu.make_async_remote_copy(
            src_ref=sbuf.at[s, pl.ds(src_at, half), :],
            dst_ref=rbuf.at[s, pl.ds(off, half), :],
            send_sem=red_send.at[s, t],
            recv_sem=red_recv.at[s, t],
            device_id=(partner,),
            device_id_type=pl.DeviceIdType.MESH,
        )

    copies = []

    def start_stage(t):
        started = []
        for s in range(6):
            if t == 0 and s < 3:
                term = dot_tn(*terms[s])
                acc[s] = term[:, : term.shape[1] // 2]
                acc[s + 3] = term[:, term.shape[1] // 2 :]
            b, partner = partner_of(orders[s][t])
            if t < halvings:
                half = total >> (t + 1)
                off = total - 2 * half
                give = pl.multiple_of(base[s] + (1 - b) * half, MIN_ROWS)
                keep = pl.multiple_of(base[s] + b * half, MIN_ROWS)
                src_at = give
            else:
                half = total >> halvings
                off = total - half + (t - halvings) * half
                give = keep = base[s]
                src_at = total + (t - halvings) * half
            sbuf[s, pl.ds(src_at, half), :] = acc[s, pl.ds(give, half), :].astype(BF16)
            c = red_copy(s, t, src_at, half, off, partner)
            c.start()
            copies.append(c)
            started.append((c, keep, half, off))
            base[s] = keep
        return started

    def finish_stage(t, started):
        for s in range(6):
            c, keep, half, off = started[s]
            c.wait_recv()
            mine = acc[s, pl.ds(keep, half), :]
            if t >= halvings:
                mine = mine.astype(BF16).astype(F32)
            acc[s, pl.ds(keep, half), :] = mine + rbuf[s, pl.ds(off, half), :].astype(F32)

    started = start_stage(0)

    s_bias[...] = jnp.sum(pre_grad.astype(F32), axis=0, keepdims=True)
    wide[...] = pre_grad.reshape(n, cpad, width)
    pack(s_pre, 0)
    exchange(3, s_bias, r_bias, shared=True)
    r_pre[me] = s_pre[me]
    r_bias[me] = s_bias[...]
    edge_out[...] = dot_nt(pre[...], w1g_ref[...]).astype(BF16)

    pieces = bits + 2
    cuts = [1 + (n - 1) * i // pieces for i in range(pieces + 1)]
    for t in range(bits):
        if t > 0:
            started = start_stage(t)
        exchange(2, s_pre, r_pre, first=cuts[t], last=cuts[t + 1])
        finish_stage(t, started)

    ag = []
    for s in range(6):
        size = total >> halvings
        abuf[s, pl.ds(base[s], size), :] = acc[s, pl.ds(base[s], size), :].astype(BF16)
    for t in reversed(range(halvings)):
        row_sends = []
        for s in range(6):
            size = total >> (t + 1)
            b, partner = partner_of(orders[s][t])
            c = pltpu.make_async_remote_copy(
                src_ref=abuf.at[s, pl.ds(base[s], size), :],
                dst_ref=abuf.at[s, pl.ds(base[s], size), :],
                send_sem=ag_send.at[s, t],
                recv_sem=ag_recv.at[s, t],
                device_id=(partner,),
                device_id_type=pl.DeviceIdType.MESH,
            )
            c.start()
            row_sends.append(c)
            ag.append(c)
            base[s] = pl.multiple_of(base[s] - b * size, MIN_ROWS)
        if t >= halvings - 2:
            i = bits + halvings - 1 - t
            exchange(2, s_pre, r_pre, first=cuts[i], last=cuts[i + 1])
        if t == 0:
            arrived(2, r_pre)
            wide[...] = jnp.zeros_like(wide)
            unpack(r_pre, 0)
            back = wide[...].reshape(slots, width)
            node = dot_tn(mhot[...], back)
            high = node.astype(BF16)
            low = (node - high.astype(F32)).astype(BF16)
            mgrad_out[...] = dot_nt(high, w1m_ref[...]) + dot_nt(low, w1m_ref[...])
            arrived(3, r_bias)
            bsum_out[...] = jnp.sum(r_bias[...], axis=0)
        for c in row_sends:
            c.wait_recv()
    for s in range(3):
        wsum_out[s, :, : abuf.shape[2]] = abuf[s]
        wsum_out[s, :, abuf.shape[2] :] = abuf[s + 3]

    for c in copies + ag:
        c.wait_send()
    left(0, r_rows)
    left(1, r_msg)
    left(2, r_pre)
    left(3, r_bias)


def final_kernel(
    scale, step, rows_ref, edge_ref, bsum_ref, mgrad_ref, wsum_any, gg, mg, wg, wm, w2g, bg, gbuf, wsum, wbuf, sems
):
    slots = rows_ref.shape[1]
    steps = gbuf.shape[0] // step
    load = pltpu.make_async_copy(wsum_any, wsum, sems.at[0])
    load.start()
    copies = [pltpu.make_async_copy(mgrad_ref, mg, sems.at[1])]
    copies[0].start()
    for i in range(steps):
        part = pl.ds(i * step, step)
        hit = (rows_ref[0:1, :] - i * step) == lax.broadcasted_iota(jnp.int32, (step, slots), 0)
        gbuf[part, :] = dot(one_hot(hit), edge_ref[...])
        c = pltpu.make_async_copy(gbuf.at[part, :], gg.at[part, :], sems.at[5 + i])
        c.start()
        copies.append(c)
    load.wait()
    for s, out in enumerate((wg, wm, w2g)):
        wbuf[s] = wsum[s].astype(F32) * scale
        c = pltpu.make_async_copy(wbuf.at[s], out, sems.at[2 + s])
        c.start()
        copies.append(c)
    bg[...] = bsum_ref[...] * scale
    for c in copies:
        c.wait()


def body(n, grid_latent, mesh_latent, mesh_cotangent, grid_rows, mesh_rows, counts, w1_grid, w1_mesh, bias_one, w2):
    slot_count = grid_rows.shape[0]
    cap = slot_count // n
    cpad = -(-cap // 16) * 16
    lanes = -(-cpad // 128) * 128
    width = mesh_latent.shape[1]
    hid = w1_grid.shape[1]
    grid_n = grid_latent.shape[0]
    mesh_n = mesh_latent.shape[0]
    slots = n * cpad
    bits = n.bit_length() - 1

    vm = pl.BlockSpec(memory_space=pltpu.VMEM)
    hbm = pl.BlockSpec(memory_space=pl.ANY)
    chunks = width // 128
    extra = (max(0, bits - int(math.log2(width // MIN_ROWS))) + 1) * MIN_ROWS
    edge, rows, wsum, bsum, mgrad = pl.pallas_call(
        functools.partial(main_kernel, n, cap, cpad),
        out_shape=(
            jax.ShapeDtypeStruct((slots, width), BF16),
            jax.ShapeDtypeStruct((8, slots), jnp.int32),
            jax.ShapeDtypeStruct((3, width, hid), BF16),
            jax.ShapeDtypeStruct((1, hid), F32),
            jax.ShapeDtypeStruct((mesh_n, width), F32),
        ),
        in_specs=[hbm, vm, vm, vm, vm, vm, hbm, hbm, vm, hbm],
        out_specs=(vm,) * 5,
        scratch_shapes=[
            pltpu.VMEM((grid_n, width), BF16),
            pltpu.VMEM((width, hid), BF16),
            pltpu.VMEM((width, hid), BF16),
            pltpu.VMEM((hid, width), BF16),
            pltpu.VMEM((n, 1, lanes), jnp.int32),
            pltpu.VMEM((slots, mesh_n), BF16),
            pltpu.VMEM((n, 2 * chunks * cap, 128), BF16),
            pltpu.VMEM((n, 2 * chunks * cap, 128), BF16),
            pltpu.VMEM((n, 1, lanes), jnp.int32),
            pltpu.VMEM((n, lanes), F32),
            pltpu.VMEM((n, cpad, width), BF16),
            pltpu.VMEM((slots, width), F32),
            pltpu.VMEM((slots, hid), BF16),
            pltpu.VMEM((n, chunks * cap, 128), BF16),
            pltpu.VMEM((n, chunks * cap, 128), BF16),
            pltpu.VMEM((1, hid), F32),
            pltpu.VMEM((n, 1, hid), F32),
            pltpu.VMEM((6, width, hid // 2), F32),
            pltpu.VMEM((6, width + extra, hid // 2), BF16),
            pltpu.VMEM((6, width + extra, hid // 2), BF16),
            pltpu.VMEM((6, width, hid // 2), BF16),
            pltpu.SemaphoreType.DMA,
            pltpu.SemaphoreType.DMA((3,)),
            pltpu.SemaphoreType.DMA((4,)),
            pltpu.SemaphoreType.DMA((4,)),
            pltpu.SemaphoreType.DMA((6, bits)),
            pltpu.SemaphoreType.DMA((6, bits)),
            pltpu.SemaphoreType.DMA((6, bits)),
            pltpu.SemaphoreType.DMA((6, bits)),
        ],
        compiler_params=pltpu.CompilerParams(
            collective_id=0, has_side_effects=True, vmem_limit_bytes=VMEM_LIMIT
        ),
    )(
        grid_latent,
        mesh_latent,
        mesh_cotangent,
        grid_rows,
        mesh_rows,
        counts,
        w1_grid,
        w1_mesh,
        bias_one.reshape(1, hid),
        w2,
    )

    step = min(512, grid_n)
    steps = grid_n // step
    scale = 1.0 / math.sqrt(n * slot_count)
    gg, mg, wg, wm, w2g, bg = pl.pallas_call(
        functools.partial(final_kernel, scale, step),
        out_shape=(
            jax.ShapeDtypeStruct((grid_n, width), F32),
            jax.ShapeDtypeStruct((mesh_n, width), F32),
            jax.ShapeDtypeStruct((width, hid), F32),
            jax.ShapeDtypeStruct((width, hid), F32),
            jax.ShapeDtypeStruct((width, hid), F32),
            jax.ShapeDtypeStruct((1, hid), F32),
        ),
        in_specs=[vm, vm, vm, vm, hbm],
        out_specs=(hbm, hbm, hbm, hbm, hbm, vm),
        scratch_shapes=[
            pltpu.VMEM((grid_n, width), F32),
            pltpu.VMEM((3, width, hid), BF16),
            pltpu.VMEM((3, width, hid), F32),
            pltpu.SemaphoreType.DMA((5 + steps,)),
        ],
        compiler_params=pltpu.CompilerParams(vmem_limit_bytes=VMEM_LIMIT),
    )(rows, edge, bsum, mgrad, wsum)
    return gg, mg, wg, wm, w2g, bg.reshape(hid)


def solution(mesh):
    return jax.shard_map(
        functools.partial(body, mesh.shape["patch"]),
        mesh=mesh,
        in_specs=(
            P("patch", None),
            P("patch", None),
            P("patch", None),
            P("patch"),
            P("patch"),
            P("patch", None),
            P(),
            P(),
            P(),
            P(),
        ),
        out_specs=(P("patch", None), P("patch", None), P(), P(), P(), P()),
        check_vma=False,
    )
```

```python
import functools
import math

import jax
import jax.numpy as jnp
from jax import lax
from jax.experimental import pallas as pl
from jax.experimental.pallas import tpu as pltpu
from jax.sharding import PartitionSpec as P

BF16 = jnp.bfloat16
F32 = jnp.float32
VMEM_LIMIT = 64 * 1024 * 1024 - 1024 * 1024
MIN_ROWS = 16


def dot(a, b):
    return jnp.dot(a, b, preferred_element_type=F32)


def dot_tn(a, b):
    return lax.dot_general(a, b, (((0,), (0,)), ((), ())), preferred_element_type=F32)


def dot_nt(a, b):
    return lax.dot_general(a, b, (((1,), (1,)), ((), ())), preferred_element_type=F32)


def one_hot(hit):
    return jnp.where(hit, 1.0, 0.0).astype(BF16)


def bit_orders(bits):
    if bits < 4:
        return [list(range(bits))] * 3
    rest = list(range(4, bits))
    return [[0, *order, *rest] for order in ((1, 2, 3), (2, 3, 1), (3, 1, 2))]


def main_kernel(
    n,
    cap,
    cpad,
    grid_any,
    mesh_ref,
    cot_ref,
    grows_ref,
    mrows_ref,
    counts_ref,
    w1g_any,
    w1m_any,
    bias_ref,
    w2_any,
    edge_out,
    rows_out,
    wsum_out,
    bsum_out,
    mgrad_out,
    glat,
    w1g_ref,
    w1m_ref,
    w2_ref,
    s_rows,
    mhot,
    s_msg,
    r_msg,
    r_rows,
    rows2,
    wide,
    gin,
    pre,
    s_pre,
    r_pre,
    s_bias,
    r_bias,
    acc,
    sbuf,
    rbuf,
    abuf,
    edge_buf,
    mgrad_buf,
    out_sem,
    glat_sem,
    weight_sem,
    phase_send,
    phase_recv,
    red_send,
    red_recv,
    ag_send,
    ag_recv,
):
    me = lax.axis_index("patch")
    width = mesh_ref.shape[1]
    slots = n * cpad
    grid_rows_n = glat.shape[0]
    mesh_n = mesh_ref.shape[0]

    load = pltpu.make_async_copy(grid_any, glat, glat_sem)
    loads = [
        pltpu.make_async_copy(src, dst, weight_sem.at[i])
        for i, (src, dst) in enumerate(((w1g_any, w1g_ref), (w1m_any, w1m_ref), (w2_any, w2_ref)))
    ]

    barrier = pltpu.get_barrier_semaphore()

    def greet(k, carry):
        pl.semaphore_signal(barrier, inc=1, device_id=(lax.rem(me + k, n),), device_id_type=pl.DeviceIdType.MESH)
        return carry

    lax.fori_loop(1, n, greet, 0)

    for c in loads:
        c.start()
    load.start()

    lanes = rows2.shape[1]
    count = grows_ref.shape[0]
    chunks = width // 128
    slot_id = lax.broadcasted_iota(jnp.int32, (slots, 1), 0)
    slot_patch = slot_id // cpad
    slot_in = slot_id % cpad
    at = lax.broadcasted_iota(jnp.int32, (n, count), 1) - cap * lax.broadcasted_iota(jnp.int32, (n, count), 0)
    own_part = (at >= 0) & (at < cap)
    lane_of = lax.broadcasted_iota(jnp.int32, (count, lanes), 0) % cap == lax.broadcasted_iota(jnp.int32, (count, lanes), 1)
    lane_of = jnp.where(lane_of, 1.0, 0.0)
    in_cap = lax.broadcasted_iota(jnp.int32, (n, lanes), 1) < cap
    from_patch = jnp.where(slot_patch == lax.broadcasted_iota(jnp.int32, (slots, n), 1), 1.0, 0.0)
    own_lane = lax.broadcasted_iota(jnp.int32, (slots, lanes), 1) == slot_in

    def table_of(ref):
        spread = jnp.where(own_part, ref[...].reshape(1, count).astype(F32), 0.0)
        out = jnp.dot(spread, lane_of, preferred_element_type=F32, precision=lax.Precision.HIGHEST)
        return jnp.where(in_cap, out, -1.0)

    def column_of(table):
        spread = jnp.dot(from_patch, table, preferred_element_type=F32, precision=lax.Precision.HIGHEST)
        return jnp.sum(jnp.where(own_lane, spread, 0.0), axis=1, keepdims=True).astype(jnp.int32)

    rows2[...] = table_of(grows_ref)

    def split(p, carry):
        s_rows[p] = rows2[pl.ds(p, 1), :].astype(jnp.int32)
        return carry

    lax.fori_loop(0, n, split, 0)
    mcol = column_of(table_of(mrows_ref))
    counted = jnp.where(
        slot_patch == lax.broadcasted_iota(jnp.int32, (slots, n), 1), counts_ref[...].astype(F32), 0.0
    )
    live = slot_in.astype(F32) < jnp.sum(counted, axis=1, keepdims=True)
    lcol = jnp.where(live, mcol, -1)
    mesh_iota = lax.broadcasted_iota(jnp.int32, (slots, mesh_n), 1)
    mhot[...] = one_hot(mcol == mesh_iota)

    def pack(ref, first):
        for j in range(chunks):
            ref[:, (first + j) * cap : (first + j + 1) * cap, :] = wide[:, 0:cap, j * 128 : (j + 1) * 128]

    def unpack(ref, first):
        for j in range(chunks):
            wide[:, 0:cap, j * 128 : (j + 1) * 128] = ref[:, (first + j) * cap : (first + j + 1) * cap, :]

    wide[...] = dot(mhot[...], mesh_ref[...]).astype(BF16).reshape(n, cpad, width)
    pack(s_msg, 0)
    wide[...] = dot(one_hot(lcol == mesh_iota), cot_ref[...]).astype(BF16).reshape(n, cpad, width)
    pack(s_msg, chunks)

    pl.semaphore_wait(barrier, n - 1)

    def exchange(phase, src, dst, shared=False, first=1, last=n):
        def send(k, carry):
            partner = lax.rem(me + k, n)
            pltpu.make_async_remote_copy(
                src_ref=src if shared else src.at[partner],
                dst_ref=dst.at[me],
                send_sem=phase_send.at[phase],
                recv_sem=phase_recv.at[phase],
                device_id=(partner,),
                device_id_type=pl.DeviceIdType.MESH,
            ).start()
            return carry

        lax.fori_loop(first, last, send, 0)

    def arrived(phase, dst):
        part = dst.at[pl.ds(0, n - 1)]
        pltpu.make_async_copy(part, part, phase_recv.at[phase]).wait()

    def left(phase, dst):
        part = dst.at[pl.ds(0, n - 1)]
        pltpu.make_async_copy(part, part, phase_send.at[phase]).wait()

    exchange(0, s_rows, r_rows)
    exchange(1, s_msg, r_msg)
    r_rows[me] = s_rows[me]
    r_msg[me] = s_msg[me]
    arrived(0, r_rows)

    def flatten(p, carry):
        rows2[pl.ds(p, 1), :] = r_rows[p].astype(F32)
        return carry

    lax.fori_loop(0, n, flatten, 0)
    table = rows2[...]
    col = column_of(table)
    to_patch = jnp.where(
        lax.broadcasted_iota(jnp.int32, (n, slots), 1) // cpad == lax.broadcasted_iota(jnp.int32, (n, slots), 0), 1.0, 0.0
    )
    spread_t = lax.dot_general(
        table, to_patch, (((0,), (0,)), ((), ())), preferred_element_type=F32, precision=lax.Precision.HIGHEST
    )
    own_sub = lax.broadcasted_iota(jnp.int32, (lanes, slots), 0) == lax.broadcasted_iota(jnp.int32, (lanes, slots), 1) % cpad
    row = jnp.sum(jnp.where(own_sub, spread_t, 0.0), axis=0, keepdims=True).astype(jnp.int32)
    rows_out[...] = jnp.broadcast_to(row, rows_out.shape)

    load.wait()
    for c in loads:
        c.wait()
    step = min(512, grid_rows_n)
    gin[...] = jnp.zeros_like(gin)

    def gather(i, carry):
        base = pl.multiple_of(i * step, step)
        hit = (col - base) == lax.broadcasted_iota(jnp.int32, (slots, step), 1)
        gin[...] += dot(one_hot(hit), glat[pl.ds(base, step), :])
        return carry

    lax.fori_loop(0, grid_rows_n // step, gather, 0)
    grid_in = gin[...].astype(BF16)
    grid_proj = dot(grid_in, w1g_ref[...]).astype(BF16).astype(F32)

    arrived(1, r_msg)
    wide[...] = jnp.zeros_like(wide)
    unpack(r_msg, chunks)
    out_grad = wide[...].reshape(slots, width)
    unpack(r_msg, 0)
    mesh_all = wide[...].reshape(slots, width)
    before = grid_proj + dot(mesh_all, w1m_ref[...]) + bias_ref[...]
    logistic = jax.nn.sigmoid(before)
    hidden = (before * logistic).astype(BF16)
    derivative = logistic * (1.0 + before * (1.0 - logistic))
    pre_f = dot_nt(out_grad, w2_ref[...]) * derivative
    pre_grad = pre_f.astype(BF16)
    pre[...] = pre_grad

    terms = ((grid_in, pre_grad), (mesh_all, pre_grad), (hidden, out_grad))

    bits = n.bit_length() - 1
    orders = bit_orders(bits)
    total = acc.shape[1]
    halvings = 0
    while halvings < bits and (total >> (halvings + 1)) >= MIN_ROWS:
        halvings += 1
    base = [0] * 3

    def partner_of(bit):
        b = lax.rem(me // (1 << bit), 2)
        return b, me + (1 - 2 * b) * (1 << bit)

    def red_copy(s, t, src_at, half, off, partner):
        return pltpu.make_async_remote_copy(
            src_ref=sbuf.at[s, pl.ds(src_at, half), :],
            dst_ref=rbuf.at[s, pl.ds(off, half), :],
            send_sem=red_send.at[s, t],
            recv_sem=red_recv.at[s, t],
            device_id=(partner,),
            device_id_type=pl.DeviceIdType.MESH,
        )

    copies = []

    def start_stage(t):
        started = []
        for s in range(3):
            if t == 0:
                acc[s] = dot_tn(*terms[s])
            b, partner = partner_of(orders[s][t])
            if t < halvings:
                half = total >> (t + 1)
                off = total - 2 * half
                give = pl.multiple_of(base[s] + (1 - b) * half, MIN_ROWS)
                keep = pl.multiple_of(base[s] + b * half, MIN_ROWS)
                src_at = give
            else:
                half = total >> halvings
                off = total - half + (t - halvings) * half
                give = keep = base[s]
                src_at = total + (t - halvings) * half
            sbuf[s, pl.ds(src_at, half), :] = acc[s, pl.ds(give, half), :].astype(BF16)
            c = red_copy(s, t, src_at, half, off, partner)
            c.start()
            copies.append(c)
            started.append((c, keep, half, off))
            base[s] = keep
        return started

    def finish_stage(t, started):
        for s in range(3):
            c, keep, half, off = started[s]
            c.wait_recv()
            mine = acc[s, pl.ds(keep, half), :]
            if t >= halvings:
                mine = mine.astype(BF16).astype(F32)
            acc[s, pl.ds(keep, half), :] = mine + rbuf[s, pl.ds(off, half), :].astype(F32)

    started = start_stage(0)

    s_bias[...] = jnp.sum(pre_grad.astype(F32), axis=0, keepdims=True)
    wide[...] = pre_grad.reshape(n, cpad, width)
    pack(s_pre, 0)
    exchange(3, s_bias, r_bias, shared=True)
    r_pre[me] = s_pre[me]
    r_bias[me] = s_bias[...]
    edge_buf[...] = dot_nt(pre[...], w1g_ref[...]).astype(BF16)
    outs = [pltpu.make_async_copy(edge_buf, edge_out, out_sem.at[0])]
    outs[0].start()

    pieces = bits + 2
    cuts = [1 + (n - 1) * i // pieces for i in range(pieces + 1)]
    for t in range(bits):
        if t > 0:
            started = start_stage(t)
        exchange(2, s_pre, r_pre, first=cuts[t], last=cuts[t + 1])
        finish_stage(t, started)

    ag = []
    for s in range(3):
        size = total >> halvings
        abuf[s, pl.ds(base[s], size), :] = acc[s, pl.ds(base[s], size), :].astype(BF16)
    for t in reversed(range(halvings)):
        row_sends = []
        for s in range(3):
            size = total >> (t + 1)
            b, partner = partner_of(orders[s][t])
            c = pltpu.make_async_remote_copy(
                src_ref=abuf.at[s, pl.ds(base[s], size), :],
                dst_ref=abuf.at[s, pl.ds(base[s], size), :],
                send_sem=ag_send.at[s, t],
                recv_sem=ag_recv.at[s, t],
                device_id=(partner,),
                device_id_type=pl.DeviceIdType.MESH,
            )
            c.start()
            row_sends.append(c)
            ag.append(c)
            base[s] = pl.multiple_of(base[s] - b * size, MIN_ROWS)
        if t >= halvings - 2:
            i = bits + halvings - 1 - t
            exchange(2, s_pre, r_pre, first=cuts[i], last=cuts[i + 1])
        if t == 0:
            arrived(2, r_pre)
            wide[...] = jnp.zeros_like(wide)
            unpack(r_pre, 0)
            back = wide[...].reshape(slots, width)
            node = dot_tn(mhot[...], back)
            high = node.astype(BF16)
            low = (node - high.astype(F32)).astype(BF16)
            mgrad_buf[...] = dot_nt(high, w1m_ref[...]) + dot_nt(low, w1m_ref[...])
            outs.append(pltpu.make_async_copy(mgrad_buf, mgrad_out, out_sem.at[1]))
            outs[1].start()
            arrived(3, r_bias)
            bsum_out[...] = jnp.sum(r_bias[...], axis=0)
        for c in row_sends:
            c.wait_recv()
    outs.append(pltpu.make_async_copy(abuf, wsum_out, out_sem.at[2]))
    outs[2].start()

    for c in copies + ag:
        c.wait_send()
    left(0, r_rows)
    left(1, r_msg)
    left(2, r_pre)
    left(3, r_bias)
    for c in outs:
        c.wait()


def final_kernel(
    scale, step, rows_ref, edge_ref, bsum_ref, mgrad_ref, wsum_any, gg, mg, wg, wm, w2g, bg, gbuf, wsum, wbuf, sems
):
    slots = rows_ref.shape[1]
    steps = gbuf.shape[0] // step
    load = pltpu.make_async_copy(wsum_any, wsum, sems.at[0])
    load.start()
    copies = [pltpu.make_async_copy(mgrad_ref, mg, sems.at[1])]
    copies[0].start()
    for i in range(steps):
        part = pl.ds(i * step, step)
        hit = (rows_ref[0:1, :] - i * step) == lax.broadcasted_iota(jnp.int32, (step, slots), 0)
        gbuf[part, :] = dot(one_hot(hit), edge_ref[...])
        c = pltpu.make_async_copy(gbuf.at[part, :], gg.at[part, :], sems.at[5 + i])
        c.start()
        copies.append(c)
    load.wait()
    for s, out in enumerate((wg, wm, w2g)):
        wbuf[s] = wsum[s].astype(F32) * scale
        c = pltpu.make_async_copy(wbuf.at[s], out, sems.at[2 + s])
        c.start()
        copies.append(c)
    bg[...] = bsum_ref[...] * scale
    for c in copies:
        c.wait()


def body(n, grid_latent, mesh_latent, mesh_cotangent, grid_rows, mesh_rows, counts, w1_grid, w1_mesh, bias_one, w2):
    slot_count = grid_rows.shape[0]
    cap = slot_count // n
    cpad = -(-cap // 16) * 16
    lanes = -(-cpad // 128) * 128
    width = mesh_latent.shape[1]
    hid = w1_grid.shape[1]
    grid_n = grid_latent.shape[0]
    mesh_n = mesh_latent.shape[0]
    slots = n * cpad
    bits = n.bit_length() - 1

    vm = pl.BlockSpec(memory_space=pltpu.VMEM)
    hbm = pl.BlockSpec(memory_space=pl.ANY)
    chunks = width // 128
    extra = (max(0, bits - int(math.log2(width // MIN_ROWS))) + 1) * MIN_ROWS
    edge, rows, wsum, bsum, mgrad = pl.pallas_call(
        functools.partial(main_kernel, n, cap, cpad),
        out_shape=(
            jax.ShapeDtypeStruct((slots, width), BF16),
            jax.ShapeDtypeStruct((8, slots), jnp.int32),
            jax.ShapeDtypeStruct((3, width, hid), BF16),
            jax.ShapeDtypeStruct((1, hid), F32),
            jax.ShapeDtypeStruct((mesh_n, width), F32),
        ),
        in_specs=[hbm, vm, vm, vm, vm, vm, hbm, hbm, vm, hbm],
        out_specs=(hbm, vm, hbm, vm, hbm),
        scratch_shapes=[
            pltpu.VMEM((grid_n, width), BF16),
            pltpu.VMEM((width, hid), BF16),
            pltpu.VMEM((width, hid), BF16),
            pltpu.VMEM((hid, width), BF16),
            pltpu.VMEM((n, 1, lanes), jnp.int32),
            pltpu.VMEM((slots, mesh_n), BF16),
            pltpu.VMEM((n, 2 * chunks * cap, 128), BF16),
            pltpu.VMEM((n, 2 * chunks * cap, 128), BF16),
            pltpu.VMEM((n, 1, lanes), jnp.int32),
            pltpu.VMEM((n, lanes), F32),
            pltpu.VMEM((n, cpad, width), BF16),
            pltpu.VMEM((slots, width), F32),
            pltpu.VMEM((slots, hid), BF16),
            pltpu.VMEM((n, chunks * cap, 128), BF16),
            pltpu.VMEM((n, chunks * cap, 128), BF16),
            pltpu.VMEM((1, hid), F32),
            pltpu.VMEM((n, 1, hid), F32),
            pltpu.VMEM((3, width, hid), F32),
            pltpu.VMEM((3, width + extra, hid), BF16),
            pltpu.VMEM((3, width + extra, hid), BF16),
            pltpu.VMEM((3, width, hid), BF16),
            pltpu.VMEM((slots, width), BF16),
            pltpu.VMEM((mesh_n, width), F32),
            pltpu.SemaphoreType.DMA((3,)),
            pltpu.SemaphoreType.DMA,
            pltpu.SemaphoreType.DMA((3,)),
            pltpu.SemaphoreType.DMA((4,)),
            pltpu.SemaphoreType.DMA((4,)),
            pltpu.SemaphoreType.DMA((3, bits)),
            pltpu.SemaphoreType.DMA((3, bits)),
            pltpu.SemaphoreType.DMA((3, bits)),
            pltpu.SemaphoreType.DMA((3, bits)),
        ],
        compiler_params=pltpu.CompilerParams(
            collective_id=0, has_side_effects=True, vmem_limit_bytes=VMEM_LIMIT
        ),
    )(
        grid_latent,
        mesh_latent,
        mesh_cotangent,
        grid_rows,
        mesh_rows,
        counts,
        w1_grid,
        w1_mesh,
        bias_one.reshape(1, hid),
        w2,
    )

    step = min(512, grid_n)
    steps = grid_n // step
    scale = 1.0 / math.sqrt(n * slot_count)
    gg, mg, wg, wm, w2g, bg = pl.pallas_call(
        functools.partial(final_kernel, scale, step),
        out_shape=(
            jax.ShapeDtypeStruct((grid_n, width), F32),
            jax.ShapeDtypeStruct((mesh_n, width), F32),
            jax.ShapeDtypeStruct((width, hid), F32),
            jax.ShapeDtypeStruct((width, hid), F32),
            jax.ShapeDtypeStruct((width, hid), F32),
            jax.ShapeDtypeStruct((1, hid), F32),
        ),
        in_specs=[vm, vm, vm, vm, hbm],
        out_specs=(hbm, hbm, hbm, hbm, hbm, vm),
        scratch_shapes=[
            pltpu.VMEM((grid_n, width), F32),
            pltpu.VMEM((3, width, hid), BF16),
            pltpu.VMEM((3, width, hid), F32),
            pltpu.SemaphoreType.DMA((5 + steps,)),
        ],
        compiler_params=pltpu.CompilerParams(vmem_limit_bytes=VMEM_LIMIT),
    )(rows, edge, bsum, mgrad, wsum)
    return gg, mg, wg, wm, w2g, bg.reshape(hid)


def solution(mesh):
    return jax.shard_map(
        functools.partial(body, mesh.shape["patch"]),
        mesh=mesh,
        in_specs=(
            P("patch", None),
            P("patch", None),
            P("patch", None),
            P("patch"),
            P("patch"),
            P("patch", None),
            P(),
            P(),
            P(),
            P(),
        ),
        out_specs=(P("patch", None), P("patch", None), P(), P(), P(), P()),
        check_vma=False,
    )
```
